128 devices in a mesh: freq: 4 (over z), trace: 32 (over y, x, core).
Axes of the slice: x: 4, y: 4, z: 4, core: 2. Of those that a mesh axis runs over, the one named last changes fastest.
Arguments:
- recorded: float32 [8, 2, 2048, 4096], P(None, None, 'freq', 'trace'), may hold values from -16 to 16
- multiples: float32 [8, 2, 2048, 4096], P(None, None, 'freq', 'trace'), may hold values from -6 to 6
Outputs:
- primaries: float32 [8, 2, 2048, 4096], P(None, None, 'freq', 'trace')
- filters: float32 [8, 2, 32, 64], P(None, None, 'freq')
The draws below stay inside these ranges and needn't reach their ends.
All inputs are finite; a program needn't handle non-finite values.
Results may differ from the reference program's by a relative error of at most 0.0001.
Values sent between devices are 32-bit elements; how exact they have to be, the bound alone decides.
No kernel may reach another device: no remote copies, remote signals or barrier semaphores. Data moves between devices by JAX's collectives and lax.ppermute only.
A program may use at most 128 MiB of HBM per device.

```python
import jax
import jax.numpy as jnp
from jax import lax

SHOTS = 8
NF = 2048
FB = 64
TAPS = 64
ITERS = 3
NX = 4096
NB = 32
N_TRACE = 32


def paired_fields(key):
    key_mult, key_smooth, key_noise, key_first, key_second = jax.random.split(jax.random.fold_in(key, 17), 5)
    white_part = jax.random.normal(key_mult, (SHOTS, 2, NF, NX), jnp.float32)
    base_field = jax.random.normal(key_smooth, (SHOTS, 2, NF, NX), jnp.float32)
    smooth_part = base_field
    for offset in range(1, 12):
        smooth_part = smooth_part + jnp.roll(base_field, offset, axis=3)
    smooth_part = smooth_part * 0.28867513
    mult_field = jnp.clip((white_part + 2.0 * smooth_part) * 0.4472136, -6.0, 6.0)
    noise_part = jnp.clip(jax.random.normal(key_noise, (SHOTS, 2, NF, NX), jnp.float32), -4.0, 4.0)
    first_gain = jax.random.uniform(key_first, (SHOTS, 2, NF, 1), jnp.float32, -1.0, 1.0)
    second_gain = jax.random.uniform(key_second, (SHOTS, 2, NF, 1), jnp.float32, -0.6, 0.6)
    shifted = jnp.roll(mult_field, 1, axis=3)
    real_part = first_gain[:, 0] * mult_field[:, 0] - first_gain[:, 1] * mult_field[:, 1] + second_gain[:, 0] * shifted[:, 0] - second_gain[:, 1] * shifted[:, 1]
    imag_part = first_gain[:, 0] * mult_field[:, 1] + first_gain[:, 1] * mult_field[:, 0] + second_gain[:, 0] * shifted[:, 1] + second_gain[:, 1] * shifted[:, 0]
    recorded_field = jnp.clip(noise_part + jnp.stack([real_part, imag_part], axis=1), -16.0, 16.0)
    return (recorded_field, mult_field)


def draw_recorded(key, part):
    return paired_fields(key)[0]


def draw_multiples(key, part):
    return paired_fields(key)[1]


def setup_inputs(seed: int = 0) -> dict:
    key_of = jax.random.split(jax.random.key(seed), 3)
    recorded = draw_recorded(jax.random.fold_in(key_of[2], 71), 0)
    multiples = draw_multiples(jax.random.fold_in(key_of[2], 71), 0)
    return dict(recorded=recorded, multiples=multiples)


def toeplitz_rows(taps_vec, trace_rows):
    tap_count = taps_vec.shape[-1]
    window_len = trace_rows + tap_count
    leading = taps_vec.shape[:-1]
    padded = jnp.concatenate([jnp.zeros(leading + (1,), jnp.float32), taps_vec[..., ::-1], jnp.zeros(leading + (trace_rows,), jnp.float32)], -1)
    repeated = jnp.tile(padded, (1,) * len(leading) + (trace_rows,))
    return repeated[..., :trace_rows * window_len].reshape(leading + (trace_rows, window_len))


def product(left, right):
    return jnp.einsum('bfj,bxj->bfx', left, right, precision=lax.Precision.HIGHEST)


def correlate(left, right):
    return jnp.einsum('bfj,bfx->bxj', left, right, precision=lax.Precision.HIGHEST)


def forward_one(window, taps_vec):
    trace_rows = window.shape[-1] - taps_vec.shape[-1]
    toeplitz = toeplitz_rows(taps_vec, trace_rows)
    real_part = product(window[0], toeplitz[0]) - product(window[1], toeplitz[1])
    imag_part = product(window[0], toeplitz[1]) + product(window[1], toeplitz[0])
    return jnp.stack([real_part, imag_part])


def adjoint_one(window, residual, tap_count):
    real_part = correlate(window[0], residual[0]) + correlate(window[1], residual[1])
    imag_part = correlate(window[0], residual[1]) - correlate(window[1], residual[0])
    crossed = jnp.stack([real_part, imag_part])
    trace_rows, window_len = crossed.shape[-2:]
    leading = crossed.shape[:-2]
    flattened = crossed.reshape(leading + (trace_rows * window_len,))
    flattened = jnp.concatenate([flattened, jnp.zeros(leading + (trace_rows,), jnp.float32)], -1)
    column_sums = jnp.sum(flattened.reshape(leading + (trace_rows, window_len + 1)), axis=-2)
    return column_sums[..., 1:tap_count + 1][..., ::-1]


def reference(recorded, multiples):
    half_taps = TAPS // 2
    tile_rows = NX // N_TRACE
    window_len = tile_rows + TAPS
    padded = jnp.pad(multiples, ((0, 0), (0, 0), (0, 0), (half_taps, half_taps)))
    tiles_all = jnp.stack([padded[..., tile_index * tile_rows: tile_index * tile_rows + window_len] for tile_index in range(N_TRACE)])
    tiles_all = tiles_all.reshape(N_TRACE, SHOTS, 2, NB, FB, window_len)
    weight = 0.5 * FB * NX

    def forward(shaping):
        result = lax.map(lambda tile: lax.map(lambda paired: forward_one(paired[0], paired[1]), (tile, shaping)), tiles_all)
        return jnp.moveaxis(result, 0, 4).reshape(SHOTS, 2, NF, NX)

    def adjoint(residual):
        pieces = jnp.moveaxis(residual.reshape(SHOTS, 2, NB, FB, N_TRACE, tile_rows), 4, 0)
        result = lax.map(lambda paired: lax.map(lambda inner_pair: adjoint_one(inner_pair[0], inner_pair[1], TAPS), paired), (tiles_all, pieces))
        return jnp.sum(result, axis=0)

    def bending(vector):
        edge_pad = jnp.pad(vector, ((0, 0), (0, 0), (1, 1), (0, 0)))
        return 2.0 * vector - edge_pad[:, :, :-2] - edge_pad[:, :, 2:]

    def inner_sum(left, right):
        return jnp.sum(left * right, axis=(1, 2, 3))

    shaping = jnp.zeros((SHOTS, 2, NB, TAPS), jnp.float32)
    bent_sum = jnp.zeros((SHOTS, 2, NB, TAPS), jnp.float32)
    residual = recorded
    direction = shaping
    norm_now = jnp.ones((SHOTS,), jnp.float32)
    for iteration in range(ITERS):
        gradient = adjoint(residual) - bent_sum
        norm_next = inner_sum(gradient, gradient)
        if iteration == 0:
            direction = gradient
        else:
            direction = gradient + (norm_next / norm_now)[:, None, None, None] * direction
        norm_now = norm_next
        applied = forward(direction)
        smooth = weight * bending(direction)
        energy = inner_sum(applied, applied) + inner_sum(direction, smooth)
        step_len = (norm_now / energy)[:, None, None, None]
        shaping = shaping + step_len * direction
        residual = residual - step_len * applied
        bent_sum = bent_sum + step_len * smooth
    return residual, shaping
```

```python
import jax
import jax.numpy as jnp
from jax import lax
from jax.experimental import pallas as pl
from jax.experimental.pallas import tpu as pltpu
from jax.sharding import Mesh
from jax.sharding import PartitionSpec as P

FB = 64
TAPS = 64
ITERS = 3
HALF = 32
LANES = 128
EROWS = 32
GROWS = 8
AXES = ("z", "y", "x", "c")
TRACE = ("y", "x", "c")

f32 = jnp.float32
bf16 = jnp.bfloat16


def split(value):
    high = value.astype(bf16)
    return high, (value - high.astype(f32)).astype(bf16)


def mm(left, right):
    return lax.dot_general(left, right, (((1,), (0,)), ((), ())), preferred_element_type=f32)


def mm3(left, right):
    return mm(left[0], right[0]) + mm(left[0], right[1]) + mm(left[1], right[0])


def iota(shape, axis):
    return lax.broadcasted_iota(jnp.int32, shape, axis)


def paired(real, imag, low):
    half = LANES // 2
    if low == 0:
        top = (real, pltpu.roll(imag, half, 1))
        bottom = (imag, -pltpu.roll(real, half, 1))
    else:
        top = (pltpu.roll(real, half, 1), imag)
        bottom = (pltpu.roll(imag, half, 1), -real)
    left = iota(real.shape, 1) < half
    return jnp.concatenate([jnp.where(left, *top), jnp.where(left, *bottom)], axis=0)


def pack_kernel(flag_ref, m_ref, left_ref, right_ref, edge_ref):
    for b in range(8):
        rows = pl.ds(b * FB, FB)
        real, imag = m_ref[0, 0, rows, :], m_ref[0, 1, rows, :]
        turned = jnp.concatenate([real, imag], axis=0).T
        first, last = turned[:HALF], turned[LANES - HALF :]
        left_ref[0, b] = first
        right_ref[0, b] = last
        near = mm3(split(first), split(paired(real, imag, 0)))
        far = mm3(split(last), split(paired(real, imag, 1)))
        lane = iota(near.shape, 1) % 64
        edge_ref[0, b] = jnp.where(lane < HALF, near, far) * flag_ref[...]


def pack(flag, multiples):
    shots = multiples.shape[0]
    edge = pl.BlockSpec((1, 8, HALF, LANES), lambda s: (s, 0, 0, 0))
    shape = jax.ShapeDtypeStruct((shots, 8, HALF, LANES), f32)
    return pl.pallas_call(
        pack_kernel,
        grid=(shots,),
        in_specs=[
            pl.BlockSpec((1, LANES), lambda s: (0, 0)),
            pl.BlockSpec((1, 2, 512, LANES), lambda s: (s, 0, 0, 0)),
        ],
        out_specs=[edge, edge, edge],
        out_shape=[shape, shape, shape],
        name="pack",
    )(flag, multiples)


def diagonals(table, start, offset):
    total = None
    for g in range(table.shape[0] // 8):
        part = pltpu.roll(table[g * 8 : g * 8 + 8], (offset - start - g * 8) % LANES, 1)
        total = part if total is None else total + part
    row = iota(total.shape, 0)
    for bit in (1, 2, 4):
        total = jnp.where(row // bit % 2 == 1, pltpu.roll(total, LANES - bit, 1), total)
    return jnp.sum(total, axis=0, keepdims=True)


def corr_kernel(m_ref, r_ref, left_ref, right_ref, out_ref):
    row = iota((LANES, LANES), 0)
    lane = iota((LANES, LANES), 1)
    inner = lane % 64
    band = row - inner
    grad_mask = (band >= 1) & (band <= 64)
    auto_mask = (band >= -31) & (band <= 32)
    tail_mask = ((band <= 95) & (inner < HALF))[96:]
    for b in range(8):
        rows = pl.ds(b * FB, FB)
        real, imag = m_ref[0, 0, rows, :], m_ref[0, 1, rows, :]
        turned = jnp.concatenate([real, imag], axis=0).T
        window0 = jnp.concatenate([left_ref[0, b], turned[:96]], axis=0)
        window1 = jnp.concatenate([turned[HALF:], right_ref[0, b]], axis=0)
        streamed = split(jnp.concatenate([window0, window1], axis=1))
        rec_r, rec_i = r_ref[0, 0, rows, :], r_ref[0, 1, rows, :]
        grad_w = jnp.concatenate([paired(rec_r, rec_i, 0), paired(rec_r, rec_i, 1)], axis=0)
        auto_w = jnp.concatenate([paired(real, imag, 0), paired(real, imag, 1)], axis=0)
        table = mm3(streamed, split(jnp.concatenate([grad_w, auto_w], axis=1)))
        grad, auto = table[:, :LANES], table[:, LANES:]
        grad = jnp.where(grad_mask, grad, 0.0)
        main = jnp.where(auto_mask, auto, 0.0)
        tail = jnp.where(tail_mask, auto[96:], 0.0)
        out_ref[0, b, 0:1, :] = diagonals(grad, 0, 0)
        out_ref[0, b, 1:2, :] = diagonals(main, 0, HALF)
        out_ref[0, b, 2:3, :] = diagonals(tail, 96, HALF)
        out_ref[0, b, 3:8, :] = jnp.zeros((5, LANES), f32)


def corr(multiples, recorded, left, right):
    shots = multiples.shape[0]
    edge = pl.BlockSpec((1, 8, HALF, LANES), lambda s: (s, 0, 0, 0))
    field = pl.BlockSpec((1, 2, 512, LANES), lambda s: (s, 0, 0, 0))
    return pl.pallas_call(
        corr_kernel,
        grid=(shots,),
        in_specs=[field, field, edge, edge],
        out_specs=pl.BlockSpec((1, 8, GROWS, LANES), lambda s: (s, 0, 0, 0)),
        out_shape=jax.ShapeDtypeStruct((shots, 8, GROWS, LANES), f32),
        name="corr",
    )(multiples, recorded, left, right)


def reverse_lanes(value):
    one = ((iota((LANES, LANES), 0) + iota((LANES, LANES), 1)) % LANES == 0).astype(f32)
    return lax.dot_general(
        value, one, (((1,), (0,)), ((), ())), precision=lax.Precision.HIGHEST,
        preferred_element_type=f32,
    )


def solve_kernel(weight, blocks, grad_ref, main_ref, tail_ref, edge_ref, out_ref, dense, applied):
    lane = iota((blocks, LANES), 1)
    main = main_ref[...]
    tail = tail_ref[...]
    main_back = reverse_lanes(main)
    tail_back = reverse_lanes(tail)
    base_r = jnp.where(lane < 64, main + tail_back, main_back + tail)
    base_i = pltpu.roll(jnp.where(lane < 64, tail - main_back, main - tail_back), 64, 1)
    grad = pltpu.roll(reverse_lanes(grad_ref[...]), LANES - 1, 1)

    tap_lane = iota((TAPS, LANES), 1)
    edge_row = iota((HALF, LANES), 0)
    edge_lane = iota((HALF, LANES), 1)
    group_lane = edge_lane % HALF
    is_left = edge_lane % 64 < HALF
    for b in range(blocks):
        real = jnp.broadcast_to(base_r[b : b + 1], (TAPS, LANES))
        imag = jnp.broadcast_to(base_i[b : b + 1], (TAPS, LANES))
        real = pltpu.roll(real, 0, 1, stride=1, stride_axis=0)
        imag = pltpu.roll(imag, 64, 1, stride=1, stride_axis=0)
        edge = edge_ref[b]
        for step in (1, 2, 4, 8, 16):
            down = pltpu.roll(pltpu.roll(edge, step, 0), step, 1)
            up = pltpu.roll(pltpu.roll(edge, HALF - step, 0), LANES - step, 1)
            down_ok = is_left & (edge_row >= step) & (group_lane >= step)
            up_ok = (~is_left) & (edge_row < HALF - step) & (group_lane < HALF - step)
            edge = edge + jnp.where(down_ok, down, 0.0) + jnp.where(up_ok, up, 0.0)
        high = jnp.where(is_left, 0.0, pltpu.roll(edge, HALF, 1))
        low = pltpu.roll(pltpu.roll(edge, HALF - 1, 0), LANES - 33, 1)
        low = jnp.where((edge_row < HALF - 1) & (edge_lane % 64 < HALF - 1), low, 0.0)
        table = jnp.where(tap_lane < 64, real, imag)
        dense[b] = table - jnp.concatenate([low, high], axis=0)

    def apply(vector):
        columns = vector.T
        for b in range(blocks):
            part_r = columns[:TAPS, b : b + 1]
            part_i = columns[TAPS:, b : b + 1]
            table = dense[b]
            by_r = jnp.sum(table * part_r, axis=0, keepdims=True)
            by_i = jnp.sum(table * part_i, axis=0, keepdims=True)
            by_r = jnp.where(lane[:1] < 64, by_r, -by_r)
            applied[b : b + 1, :] = by_r + pltpu.roll(by_i, 64, 1)
        return applied[...]

    row = iota((blocks, LANES), 0)

    def bend(vector):
        before = jnp.where(row == 0, 0.0, pltpu.roll(vector, 1, 0))
        after = jnp.where(row == blocks - 1, 0.0, pltpu.roll(vector, blocks - 1, 0))
        return 2.0 * vector - before - after

    def inner(left, right):
        return jnp.sum(left * right, keepdims=True)

    direction = grad
    taps = jnp.zeros_like(grad)
    norm = inner(grad, grad)
    for step in range(ITERS):
        if step > 0:
            norm_next = inner(grad, grad)
            direction = grad + (norm_next / norm) * direction
            norm = norm_next
        smooth = weight * bend(direction)
        curved = apply(direction)
        energy = inner(direction, curved) + inner(direction, smooth)
        length = norm / energy
        taps = taps + length * direction
        grad = grad - length * (curved + smooth)
    out_ref[...] = pltpu.roll(reverse_lanes(taps), 63, 1)


def solve(weight, grad, main, tail, edge):
    blocks = grad.shape[0]
    return pl.pallas_call(
        lambda *refs: solve_kernel(weight, blocks, *refs),
        out_shape=jax.ShapeDtypeStruct((blocks, LANES), f32),
        scratch_shapes=[
            pltpu.VMEM((blocks, TAPS, LANES), f32),
            pltpu.VMEM((blocks, LANES), f32),
        ],
        name="solve",
    )(grad, main, tail, edge)


def subtract_kernel(m_ref, r_ref, left_ref, right_ref, taps_ref, out_ref, taps_out_ref):
    row = iota((LANES, LANES), 0)
    lane = iota((LANES, LANES), 1)
    spot = (row + HALF) % LANES
    band = spot - lane % 64
    mask = (band >= 1) & (band <= 64)
    half = iota((FB, LANES), 1) < 64
    for b in range(8):
        rows = pl.ds(b * FB, FB)
        field = jnp.concatenate([m_ref[0, 0, rows, :], m_ref[0, 1, rows, :]], axis=0)
        halo = jnp.concatenate(
            [jnp.zeros((64, LANES), f32), right_ref[0, b], left_ref[0, b]], axis=0
        ).T
        window0 = jnp.where(lane < 96, field, halo)
        window1 = jnp.where((lane < 64) | (lane >= 96), pltpu.roll(field, 64, 1), halo)
        streamed = jnp.concatenate(
            [
                jnp.concatenate([window0[:FB], window0[FB:]], axis=1),
                jnp.concatenate([window1[:FB], window1[FB:]], axis=1),
            ],
            axis=0,
        )
        streamed = jnp.concatenate(split(streamed), axis=0)
        taps = taps_ref[0, b : b + 1, :]
        swapped = pltpu.roll(taps, 64, 1)
        swapped = jnp.where(lane[:1] < 64, -swapped, swapped)
        top = jnp.broadcast_to(taps, (LANES, LANES))
        bottom = jnp.broadcast_to(swapped, (LANES, LANES))
        top = pltpu.roll(top, 96, 1, stride=1, stride_axis=0)
        bottom = pltpu.roll(bottom, 96, 1, stride=1, stride_axis=0)
        weights = jnp.concatenate(
            [jnp.where(mask, top, 0.0), jnp.where(mask, bottom, 0.0)], axis=0
        )
        weights = jnp.concatenate(split(weights), axis=1)
        made = mm(streamed, weights)
        made = (made[:LANES, :LANES] + made[LANES:, :LANES]) + (
            made[:LANES, LANES:] + made[LANES:, LANES:]
        )
        made0, made1 = made[:FB], made[FB:]
        real = jnp.where(half, made0, pltpu.roll(made1, 64, 1))
        imag = jnp.where(half, pltpu.roll(made0, 64, 1), made1)
        out_ref[0, 0, rows, :] = r_ref[0, 0, rows, :] - real
        out_ref[0, 1, rows, :] = r_ref[0, 1, rows, :] - imag
    taps_out_ref[0, 0] = taps_ref[0, :, :TAPS]
    taps_out_ref[0, 1] = taps_ref[0, :, TAPS:]


def subtract(multiples, recorded, left, right, taps):
    shots = multiples.shape[0]
    edge = pl.BlockSpec((1, 8, HALF, LANES), lambda s: (s, 0, 0, 0))
    field = pl.BlockSpec((1, 2, 512, LANES), lambda s: (s, 0, 0, 0))
    return pl.pallas_call(
        subtract_kernel,
        grid=(shots,),
        in_specs=[field, field, edge, edge, pl.BlockSpec((1, 8, LANES), lambda s: (s, 0, 0))],
        out_specs=[field, pl.BlockSpec((1, 2, 8, TAPS), lambda s: (s, 0, 0, 0))],
        out_shape=[
            jax.ShapeDtypeStruct(recorded.shape, f32),
            jax.ShapeDtypeStruct((shots, 2, 8, TAPS), f32),
        ],
        name="subtract",
    )(multiples, recorded, left, right, taps)


def body(recorded, multiples):
    shots = multiples.shape[0]
    y, x, c = (lax.axis_index(name) for name in TRACE)
    place = (y * 4 + x) * 2 + c
    lane = jnp.arange(LANES)[None] % 64
    flag = jnp.where(lane < HALF, place == 0, place == 31).astype(f32)
    first, last, edge = pack(flag, multiples)
    up = [(i, i + 1) for i in range(31)]
    left = lax.ppermute(last, TRACE, up)
    right = lax.ppermute(first, TRACE, [(j, i) for i, j in up])
    sums = corr(multiples, recorded, left, right)

    payload = jnp.concatenate([sums, edge], axis=2).reshape(2, shots // 2, 8, -1, LANES)
    mine = lax.dynamic_index_in_dim(payload, c, 0, keepdims=False)
    other = lax.dynamic_index_in_dim(payload, 1 - c, 0, keepdims=False)
    mine = mine + lax.ppermute(other, "c", [(0, 1), (1, 0)])
    rows = GROWS + EROWS
    mine = mine.reshape(16, 2 * rows, LANES)
    owned = lax.all_to_all(mine, ("y", "x"), 0, 0, tiled=True).sum(axis=0)
    shot = lax.all_to_all(
        jnp.broadcast_to(owned[None], (16, 2 * rows, LANES)), ("z", "x"), 0, 0, tiled=True
    ).reshape(32, rows, LANES)
    weight = 0.5 * FB * 4096
    taps = solve(weight, shot[:, 0], shot[:, 1], shot[:, 2], shot[:, GROWS:])
    taps = lax.dynamic_slice_in_dim(taps, lax.axis_index("z") * 8, 8, 0)
    taps = lax.all_to_all(
        jnp.broadcast_to(taps[None], (8, 8, LANES)), ("c", "y"), 0, 0, tiled=True
    )
    return tuple(subtract(multiples, recorded, left, right, taps))


def solution(mesh):
    finer = Mesh(mesh.devices.reshape(4, 4, 4, 2), AXES)
    placed = P(None, None, "z", TRACE)
    return jax.shard_map(
        body,
        mesh=finer,
        in_specs=(placed, placed),
        out_specs=(placed, P(None, None, "z", None)),
        check_vma=False,
    )
```

```python
import jax
import jax.numpy as jnp
from jax import lax
from jax.experimental import pallas as pl
from jax.experimental.pallas import tpu as pltpu
from jax.sharding import Mesh
from jax.sharding import PartitionSpec as P


FB = 64
TAPS = 64
ITERS = 3
HALF = 32
LANES = 128
AXES = ("z", "y", "x", "c")
TRACE = ("y", "x", "c")

f32 = jnp.float32
bf16 = jnp.bfloat16


def split(value):
    high = value.astype(bf16)
    return high, (value - high.astype(f32)).astype(bf16)


def mm(left, right):
    return lax.dot_general(left, right, (((1,), (0,)), ((), ())), preferred_element_type=f32)


def iota(shape, axis):
    return lax.broadcasted_iota(jnp.int32, shape, axis)


def mm_t(left, right):
    return lax.dot_general(left, right, (((1,), (1,)), ((), ())), preferred_element_type=f32)


def exact(left, right, dims):
    return lax.dot_general(
        left, right, (dims, ((), ())), precision=lax.Precision.HIGHEST,
        preferred_element_type=f32,
    )


def field_spec(first=0):
    return pl.BlockSpec((1, 2, 512, LANES), lambda s: (s + first, 0, 0, 0))


def edge_spec():
    return pl.BlockSpec((1, 8, HALF, LANES), lambda s: (s, 0, 0, 0))


def pack_kernel(m_ref, left_ref, right_ref):
    for shot in range(2):
        for b in range(8):
            rows = pl.ds(b * FB, FB)
            turned = jnp.concatenate(
                [m_ref[shot, 0, rows, :], m_ref[shot, 1, rows, :]], axis=0
            ).T
            left_ref[shot, b] = turned[:HALF]
            right_ref[shot, b] = turned[LANES - HALF :]


def pack(first, shots, multiples):
    shape = jax.ShapeDtypeStruct((shots, 8, HALF, LANES), f32)
    edge = pl.BlockSpec((2, 8, HALF, LANES), lambda s: (s, 0, 0, 0))
    return pl.pallas_call(
        pack_kernel,
        grid=(shots // 2,),
        in_specs=[pl.BlockSpec((2, 2, 512, LANES), lambda s: (s + first // 2, 0, 0, 0))],
        out_specs=[edge, edge],
        out_shape=[shape, shape],
        name="pack",
    )(multiples)


def edges_side(shots, is_left, edge_ref, out_ref):
    lane = iota((HALF, LANES), 1)
    home = (lane % 64 >= HALF) if is_left else (lane % 64 < HALF)
    spot = lane % HALF
    sign = jnp.where(lane < 64, 1.0, -1.0)

    def load(shot, b):
        if is_left:
            return edge_ref[shot, b]
        return jnp.concatenate(
            [edge_ref[shot, b, 1:, :], jnp.zeros((1, LANES), f32)], axis=0
        )

    def one(pair, carry):
        spots = [(pair * 2 + k, b) for k in range(2) for b in range(0, 8, 2)]
        tables = []
        for shot, b in spots:
            here, there = load(shot, b), load(shot, b + 1)
            here_turn = pltpu.roll(here, 64, 1) * sign
            there_turn = pltpu.roll(there, 64, 1) * sign
            if is_left:
                against = [there, here, there_turn, here_turn]
            else:
                against = [here, there, here_turn, there_turn]
            against = split(jnp.concatenate(against, axis=0))
            rows = split(jnp.concatenate([here, there], axis=0))
            made = (
                mm_t(rows[0], against[0]) + mm_t(rows[0], against[1]) + mm_t(rows[1], against[0])
            )
            tables.append(jnp.where(home, made[:HALF], made[HALF:]))
        for step in (1, 2, 4, 8, 16):
            fill = jnp.zeros((step, LANES), f32)
            inside = (spot >= step) if is_left else (spot < HALF - step)
            for k, table in enumerate(tables):
                if is_left:
                    moved = jnp.concatenate([fill, pltpu.roll(table, step, 1)[:-step]], axis=0)
                else:
                    moved = jnp.concatenate(
                        [pltpu.roll(table, LANES - step, 1)[step:], fill], axis=0
                    )
                tables[k] = table + jnp.where(inside, moved, 0.0)
        for (shot, b), table in zip(spots, tables):
            out_ref[shot, b] = jnp.where(home, table, 0.0)
            other = pltpu.roll(table, HALF if is_left else LANES - HALF, 1)
            out_ref[shot, b + 1] = jnp.where(home, other, 0.0)
        return carry

    lax.fori_loop(0, shots // 2, one, 0)


def edges_kernel(shots, on_ref, left_ref, right_ref, out_ref):
    @pl.when(on_ref[0] == 0)
    def _():
        out_ref[...] = jnp.zeros_like(out_ref)

    @pl.when(on_ref[0] == 1)
    def _():
        edges_side(shots, True, left_ref, out_ref)

    @pl.when(on_ref[0] == 2)
    def _():
        edges_side(shots, False, right_ref, out_ref)


def edges(on, first, last):
    shots = first.shape[0]
    return pl.pallas_call(
        lambda *refs: edges_kernel(shots, *refs),
        in_specs=[pl.BlockSpec(memory_space=pltpu.SMEM)]
        + [pl.BlockSpec(memory_space=pltpu.VMEM)] * 2,
        out_shape=jax.ShapeDtypeStruct((shots, 8, HALF, LANES), f32),
        name="edges",
    )(on, first, last)


def corr_kernel(shots, m_ref, r_ref, left_ref, right_ref, out_ref, high, low, w_high, w_low, acc):
    shot = pl.program_id(0)
    for b in range(8):
        rows = pl.ds(b * FB, FB)
        turned = jnp.concatenate([m_ref[0, 0, rows, :], m_ref[0, 1, rows, :]], axis=0).T
        for part, at in ((left_ref[0, b], 0), (turned, HALF), (right_ref[0, b], HALF + LANES)):
            part_high, part_low = split(part)
            high[b, pl.ds(at, part.shape[0]), :] = part_high
            low[b, pl.ds(at, part.shape[0]), :] = part_low
    left = iota((FB, LANES), 1) < 64
    for b in range(8):
        rows = pl.ds(b * FB, FB)
        for ref, at in ((r_ref, 0), (m_ref, LANES)):
            real, imag = ref[0, 0, rows, :], ref[0, 1, rows, :]
            real_turn, imag_turn = pltpu.roll(real, 64, 1), pltpu.roll(imag, 64, 1)
            pieces = (
                jnp.where(left, real, imag_turn),
                jnp.where(left, imag, -real_turn),
                jnp.where(left, real_turn, imag),
                jnp.where(left, imag_turn, -real),
            )
            for k, piece in enumerate(pieces):
                piece_high, piece_low = split(piece)
                w_high[b, pl.ds(k * FB, FB), pl.ds(at, LANES)] = piece_high
                w_low[b, pl.ds(k * FB, FB), pl.ds(at, LANES)] = piece_low
    row = iota((LANES, LANES), 0)
    inner = iota((LANES, LANES), 1) % 64
    band = row - inner
    grad_mask = (band >= 1) & (band <= 64)
    auto_mask = (band >= -31) & (band <= 32)
    tail_mask = ((band <= 95) & (inner < HALF))[96:]
    for b in range(8):
        lead = jnp.concatenate([high[b, 0:128, :], high[b, 64:192, :]], axis=1)
        rest = jnp.concatenate([low[b, 0:128, :], low[b, 64:192, :]], axis=1)
        table = mm(lead, w_high[b]) + mm(lead, w_low[b]) + mm(rest, w_high[b])
        grad, auto = table[:, :LANES], table[:, LANES:]
        for kind, part, mask, start, offset in (
            (0, grad, grad_mask, 0, 0),
            (1, auto, auto_mask, 0, HALF),
            (2, auto[96:], tail_mask, 96, HALF),
        ):
            part = jnp.where(mask, part, 0.0)
            total = None
            for g in range(part.shape[0] // 8):
                piece = pltpu.roll(part[g * 8 : g * 8 + 8], (offset - start - g * 8) % LANES, 1)
                total = piece if total is None else total + piece
            acc[kind, pl.ds(shot * 8 + b, 1)] = total[None]

    @pl.when(shot == shots - 1)
    def _():
        count = shots * 8
        sums = []
        for kind in range(3):
            total = acc[kind].reshape(count * 8, LANES)
            level = iota(total.shape, 0)
            for bit in (1, 2, 4):
                total = jnp.where(level // bit % 2 == 1, pltpu.roll(total, LANES - bit, 1), total)
            sums.append(jnp.sum(total.reshape(count, 8, LANES), axis=1))
        flip = ((iota((LANES, LANES), 0) + iota((LANES, LANES), 1)) % LANES == 0).astype(f32)
        flip = jnp.where(iota((LANES, LANES), 0) < 64, -flip, flip)
        auto = sums[1] + exact(sums[2], flip, ((1,), (0,)))
        for k in range(shots):
            out_ref[k, 0:8, :] = sums[0][k * 8 : k * 8 + 8]
            out_ref[k, 8:16, :] = auto[k * 8 : k * 8 + 8]


def corr(first, shots, multiples, recorded, left, right):
    return pl.pallas_call(
        lambda *refs: corr_kernel(shots, *refs),
        grid=(shots,),
        in_specs=[field_spec(first), field_spec(first), edge_spec(), edge_spec()],
        out_specs=pl.BlockSpec((shots, 16, LANES), lambda s: (0, 0, 0)),
        out_shape=jax.ShapeDtypeStruct((shots, 16, LANES), f32),
        scratch_shapes=[
            pltpu.VMEM((8, 192, LANES), bf16),
            pltpu.VMEM((8, 192, LANES), bf16),
            pltpu.VMEM((8, 256, 256), bf16),
            pltpu.VMEM((8, 256, 256), bf16),
            pltpu.VMEM((3, shots * 8, 8, LANES), f32),
        ],
        name="corr",
    )(multiples, recorded, left, right)


def solve_kernel(weight, z_ref, *refs):
    sums_refs, (out_ref, lags, table, vec) = refs[:4], refs[4:]
    grad_rows = jnp.concatenate([ref[0:8, :] for ref in sums_refs], axis=0)
    auto_rows = jnp.concatenate([ref[8:16, :] for ref in sums_refs], axis=0)
    turn = lambda value: pltpu.roll(value, 64, 1)
    lane = iota((TAPS, LANES), 1)
    row = iota((TAPS, LANES), 0)
    group = lane // HALF
    place = lane % HALF
    block = (place + z_ref[0] * 8) % HALF
    stacked = jnp.concatenate(
        [grad_rows, turn(grad_rows), turn(grad_rows), grad_rows], axis=0
    )
    pick = (lane == LANES - 1 - row).astype(f32)
    grad = exact(pick, stacked, ((1,), (1,)))
    lag = iota((LANES, LANES), 0) - 64
    pick = (iota((LANES, LANES), 1) == jnp.abs(lag)).astype(f32)
    stacked = jnp.concatenate(
        [auto_rows, turn(auto_rows), auto_rows, turn(auto_rows)], axis=0
    )
    made = exact(pick, stacked, ((1,), (1,)))
    odd = iota((LANES, LANES), 1) // HALF % 2 == 1
    lags[0:LANES, :] = jnp.where(odd & (lag < 0), -made, made)
    for a in range(HALF):
        part = jnp.concatenate(
            [ref[pl.ds(16 + a * 8, 8), :] for ref in sums_refs], axis=0
        )
        other = turn(part)
        turned = jnp.concatenate([part, other, part, other], axis=0).T
        table[a] = turned[:TAPS]

    flip = jnp.where(group == 3, -1.0, 1.0)
    even = group % 2 == 0

    def apply(vector):
        vec[...] = vector
        total = jnp.zeros((TAPS, LANES), f32)
        for k in range(TAPS):
            total = total + lags[64 - k : 128 - k, :] * vec[k : k + 1, :]
        low = jnp.zeros((HALF, LANES), f32)
        high = jnp.zeros((HALF, LANES), f32)
        for a in range(HALF):
            low = low + table[a, :HALF] * vec[a : a + 1, :]
            high = high + table[a, HALF:] * vec[HALF + a : HALF + a + 1, :]
        total = (total - jnp.concatenate([low, high], axis=0)) * flip
        total = total + pltpu.roll(total, LANES - HALF, 1)
        return jnp.where(even, total, pltpu.roll(total, LANES - HALF, 1))

    def bend(vector):
        before = jnp.where(place == 0, pltpu.roll(vector, 97, 1), pltpu.roll(vector, 1, 1))
        after = jnp.where(
            place == HALF - 1, pltpu.roll(vector, 31, 1), pltpu.roll(vector, 127, 1)
        )
        before = jnp.where(block == 0, 0.0, before)
        after = jnp.where(block == HALF - 1, 0.0, after)
        return 2.0 * vector - before - after

    def inner(left, right):
        return 0.5 * jnp.sum(left * right, keepdims=True)

    direction = grad
    taps = jnp.zeros_like(grad)
    norm = inner(grad, grad)
    for step in range(ITERS):
        if step > 0:
            norm_next = inner(grad, grad)
            direction = grad + (norm_next / norm) * direction
            norm = norm_next
        bent = apply(direction) + weight * bend(direction)
        length = norm / inner(direction, bent)
        taps = taps + length * direction
        grad = grad - length * bent
    pick = ((iota((TAPS, LANES), 1) % 64) == TAPS - 1 - row).astype(f32)
    made = exact(taps, pick, ((0,), (0,)))
    out_ref[...] = jnp.where(iota((8, LANES), 1) < 64, made[:8], made[HALF : HALF + 8])


def solve(weight, z, parts):
    return pl.pallas_call(
        lambda *refs: solve_kernel(weight, *refs),
        in_specs=[pl.BlockSpec(memory_space=pltpu.SMEM)]
        + [pl.BlockSpec(memory_space=pltpu.VMEM)] * 4,
        out_shape=jax.ShapeDtypeStruct((8, LANES), f32),
        scratch_shapes=[
            pltpu.VMEM((LANES, LANES), f32),
            pltpu.VMEM((HALF, TAPS, LANES), f32),
            pltpu.VMEM((TAPS, LANES), f32),
        ],
        name="solve",
    )(z, *parts)


def subtract_kernel(
    m_ref, r_ref, left_ref, right_ref, taps_ref, out_ref, taps_out_ref, lead, weights
):
    lane = iota((LANES, LANES), 1)
    for b in range(8):
        rows = pl.ds(b * FB, FB)
        field = jnp.concatenate([m_ref[0, 0, rows, :], m_ref[0, 1, rows, :]], axis=0)
        halo = jnp.concatenate(
            [jnp.zeros((64, LANES), f32), right_ref[0, b], left_ref[0, b]], axis=0
        ).T
        window0 = jnp.where(lane < 96, field, halo)
        window1 = jnp.where((lane < 64) | (lane >= 96), pltpu.roll(field, 64, 1), halo)
        for j, window in enumerate((window0, window1)):
            for k, part in enumerate(split(window)):
                at = pl.ds(k * LANES + j * FB, FB)
                lead[b, at, pl.ds(0, LANES)] = part[:FB]
                lead[b, at, pl.ds(LANES, LANES)] = part[FB:]
    spot = (iota((LANES, LANES), 0) + HALF) % LANES
    band = spot - lane % 64
    mask = (band >= 1) & (band <= 64)
    first = iota((1, LANES), 1) < 64
    for b in range(8):
        taps = taps_ref[0, b : b + 1, :]
        swapped = pltpu.roll(taps, 64, 1)
        swapped = jnp.where(first, -swapped, swapped)
        for j, line in enumerate((taps, swapped)):
            spread = jnp.broadcast_to(line, (LANES, LANES))
            spread = pltpu.roll(spread, 96, 1, stride=1, stride_axis=0)
            for k, part in enumerate(split(jnp.where(mask, spread, 0.0))):
                weights[b, pl.ds(j * LANES, LANES), pl.ds(k * LANES, LANES)] = part
    half = iota((FB, LANES), 1) < 64
    for b in range(8):
        rows = pl.ds(b * FB, FB)
        made = mm(lead[b], weights[b])
        made = (made[:LANES, :LANES] + made[LANES:, :LANES]) + (
            made[:LANES, LANES:] + made[LANES:, LANES:]
        )
        made0, made1 = made[:FB], made[FB:]
        real = jnp.where(half, made0, pltpu.roll(made1, 64, 1))
        imag = jnp.where(half, pltpu.roll(made0, 64, 1), made1)
        out_ref[0, 0, rows, :] = r_ref[0, 0, rows, :] - real
        out_ref[0, 1, rows, :] = r_ref[0, 1, rows, :] - imag
    taps_out_ref[0, 0] = taps_ref[0, :, :TAPS]
    taps_out_ref[0, 1] = taps_ref[0, :, TAPS:]


def subtract(multiples, recorded, left, right, taps):
    shots = multiples.shape[0]
    return pl.pallas_call(
        subtract_kernel,
        grid=(shots,),
        in_specs=[
            field_spec(),
            field_spec(),
            edge_spec(),
            edge_spec(),
            pl.BlockSpec((1, 8, LANES), lambda s: (s, 0, 0)),
        ],
        out_specs=[field_spec(), pl.BlockSpec((1, 2, 8, TAPS), lambda s: (s, 0, 0, 0))],
        out_shape=[
            jax.ShapeDtypeStruct(recorded.shape, f32),
            jax.ShapeDtypeStruct((shots, 2, 8, TAPS), f32),
        ],
        scratch_shapes=[
            pltpu.VMEM((8, 256, 256), bf16),
            pltpu.VMEM((8, 256, 256), bf16),
        ],
        name="subtract",
    )(multiples, recorded, left, right, taps)


def number(y, x, c):
    return (y * 4 + x) * 2 + c


def spread(value, axis, step, only=None):
    pairs = []
    for y in range(4):
        for x in range(4):
            for c in range(2):
                at = {"y": y, "x": x}
                to = dict(at)
                to[axis] = (at[axis] + step) % 4
                if only is None or only(y, x):
                    pairs.append((number(y, x, c), number(to["y"], to["x"], c)))
    return lax.ppermute(value, TRACE, pairs)


def across(value, moves):
    pairs = [
        (number(y, a, c), number(y, b, c)) for y in range(4) for a, b in moves for c in range(2)
    ]
    return lax.ppermute(value, TRACE, pairs)


def body(recorded, multiples):
    shots = multiples.shape[0]
    half = shots // 2
    y, x, c = (lax.axis_index(name) for name in TRACE)
    z = lax.axis_index("z")
    place = number(y, x, c)
    on = jnp.where(place == 0, 1, jnp.where(place == 31, 2, 0)).astype(jnp.int32)[None]
    up = [(i, i + 1) for i in range(31)]
    down = [(i + 1, i) for i in range(31)]
    first, last = pack(0, shots, multiples)
    left = lax.ppermute(last, TRACE, up)
    right = lax.ppermute(first, TRACE, down)
    ends = edges(on, first, last)

    ends = ends.reshape(2, half, 8, HALF, LANES)
    other = jnp.where(c == 0, ends[1], ends[0])
    mine = jnp.where(c == 0, ends[0], ends[1])
    mine = mine + lax.ppermute(other, TRACE, [(0, 1), (31, 30)])
    edge = lax.dynamic_index_in_dim(mine, y, 0, keepdims=False)
    for step in range(1, 4):
        sent = lax.dynamic_index_in_dim(mine, (y + step) % 4, 0, keepdims=False)
        edge = edge + spread(sent, "y", step, lambda y, x: (y, x) in ((0, 0), (3, 3)))
    edge = edge + across(edge, ((0, 2), (3, 1)))
    edge = edge + across(edge, ((0, 1), (2, 3), (3, 2), (1, 0)))
    edge = edge.transpose(1, 0, 2).reshape(8 * HALF, LANES)
    along = [[(i, (i - step) % 4) for i in range(4)] for step in range(1, 4)]

    sums = corr(0, shots, multiples, recorded, left, right)
    sums = sums.reshape(2, half, 16, LANES).swapaxes(0, 1)[:, None]
    sums = jnp.broadcast_to(sums, (4, 4, 2, 16, LANES)).reshape(32, 16, LANES)
    sums = lax.all_to_all(sums, TRACE, 0, 0, tiled=True).sum(axis=0)
    own = jnp.concatenate([sums, edge], axis=0)
    parts = [own] + [lax.ppermute(own, "z", pairs) for pairs in along]
    weight = 0.5 * FB * 4096
    taps = solve(weight, z[None], parts)
    taps = lax.all_to_all(
        jnp.broadcast_to(taps[None], (8, 8, LANES)), ("c", "y"), 0, 0, tiled=True
    )
    return tuple(subtract(multiples, recorded, left, right, taps))


def solution(mesh):
    finer = Mesh(mesh.devices.reshape(4, 4, 4, 2), AXES)
    placed = P(None, None, "z", TRACE)
    return jax.shard_map(
        body,
        mesh=finer,
        in_specs=(placed, placed),
        out_specs=(placed, P(None, None, "z", None)),
        check_vma=False,
    )
```

```python
import jax
import jax.numpy as jnp
from jax import lax
from jax.experimental import pallas as pl
from jax.experimental.pallas import tpu as pltpu
from jax.sharding import Mesh
from jax.sharding import PartitionSpec as P


FB = 64
TAPS = 64
ITERS = 3
HALF = 32
LANES = 128
AXES = ("z", "y", "x", "c")
TRACE = ("y", "x", "c")

f32 = jnp.float32
bf16 = jnp.bfloat16


def split(value):
    high = value.astype(bf16)
    return high, (value - high.astype(f32)).astype(bf16)


def mm(left, right):
    return lax.dot_general(left, right, (((1,), (0,)), ((), ())), preferred_element_type=f32)


def iota(shape, axis):
    return lax.broadcasted_iota(jnp.int32, shape, axis)


def mm_t(left, right):
    return lax.dot_general(left, right, (((1,), (1,)), ((), ())), preferred_element_type=f32)


def exact(left, right, dims):
    return lax.dot_general(
        left, right, (dims, ((), ())), precision=lax.Precision.HIGHEST,
        preferred_element_type=f32,
    )


def field_spec():
    return pl.BlockSpec((2, 2, 512, LANES), lambda s: (s, 0, 0, 0))


def edge_spec():
    return pl.BlockSpec((2, 8, HALF, LANES), lambda s: (s, 0, 0, 0))


def pack_kernel(m_ref, left_ref, right_ref):
    for shot in range(4):
        for b in range(8):
            rows = pl.ds(b * FB, FB)
            turned = jnp.concatenate(
                [m_ref[shot, 0, rows, :], m_ref[shot, 1, rows, :]], axis=0
            ).T
            left_ref[shot, b] = turned[:HALF]
            right_ref[shot, b] = turned[LANES - HALF :]


def pack(first, shots, multiples):
    shape = jax.ShapeDtypeStruct((shots, 8, HALF, LANES), f32)
    edge = pl.BlockSpec((4, 8, HALF, LANES), lambda s: (s, 0, 0, 0))
    return pl.pallas_call(
        pack_kernel,
        grid=(shots // 4,),
        in_specs=[pl.BlockSpec((4, 2, 512, LANES), lambda s: (s + first // 4, 0, 0, 0))],
        out_specs=[edge, edge],
        out_shape=[shape, shape],
        name="pack",
    )(multiples)


def edges_side(shots, is_left, edge_ref, out_ref):
    lane = iota((HALF, LANES), 1)
    home = (lane % 64 >= HALF) if is_left else (lane % 64 < HALF)
    spot = lane % HALF
    sign = jnp.where(lane < 64, 1.0, -1.0)

    def load(shot, b):
        if is_left:
            return edge_ref[shot, b]
        return jnp.concatenate(
            [edge_ref[shot, b, 1:, :], jnp.zeros((1, LANES), f32)], axis=0
        )

    def one(pair, carry):
        spots = [(pair * 2 + k, b) for k in range(2) for b in range(0, 8, 2)]
        tables = []
        for shot, b in spots:
            here, there = load(shot, b), load(shot, b + 1)
            here_turn = pltpu.roll(here, 64, 1) * sign
            there_turn = pltpu.roll(there, 64, 1) * sign
            if is_left:
                against = [there, here, there_turn, here_turn]
            else:
                against = [here, there, here_turn, there_turn]
            against = split(jnp.concatenate(against, axis=0))
            rows = split(jnp.concatenate([here, there], axis=0))
            made = (
                mm_t(rows[0], against[0]) + mm_t(rows[0], against[1]) + mm_t(rows[1], against[0])
            )
            tables.append(jnp.where(home, made[:HALF], made[HALF:]))
        for step in (1, 2, 4, 8, 16):
            fill = jnp.zeros((step, LANES), f32)
            inside = (spot >= step) if is_left else (spot < HALF - step)
            for k, table in enumerate(tables):
                if is_left:
                    moved = jnp.concatenate([fill, pltpu.roll(table, step, 1)[:-step]], axis=0)
                else:
                    moved = jnp.concatenate(
                        [pltpu.roll(table, LANES - step, 1)[step:], fill], axis=0
                    )
                tables[k] = table + jnp.where(inside, moved, 0.0)
        for (shot, b), table in zip(spots, tables):
            out_ref[shot, b] = jnp.where(home, table, 0.0)
            other = pltpu.roll(table, HALF if is_left else LANES - HALF, 1)
            out_ref[shot, b + 1] = jnp.where(home, other, 0.0)
        return carry

    lax.fori_loop(0, shots // 2, one, 0)


def edges_kernel(shots, on_ref, left_ref, right_ref, out_ref):
    @pl.when(on_ref[0] == 0)
    def _():
        out_ref[...] = jnp.zeros_like(out_ref)

    @pl.when(on_ref[0] == 1)
    def _():
        edges_side(shots, True, left_ref, out_ref)

    @pl.when(on_ref[0] == 2)
    def _():
        edges_side(shots, False, right_ref, out_ref)


def edges(on, first, last):
    shots = first.shape[0]
    return pl.pallas_call(
        lambda *refs: edges_kernel(shots, *refs),
        in_specs=[pl.BlockSpec(memory_space=pltpu.SMEM)]
        + [pl.BlockSpec(memory_space=pltpu.VMEM)] * 2,
        out_shape=jax.ShapeDtypeStruct((shots, 8, HALF, LANES), f32),
        compiler_params=pltpu.CompilerParams(vmem_limit_bytes=8 * 2**20),
        name="edges",
    )(on, first, last)


def corr_kernel(shots, m_ref, r_ref, left_ref, right_ref, out_ref, high, low, w_high, w_low, acc):
    step = pl.program_id(0)
    for b in range(16):
        rows = pl.ds(b % 8 * FB, FB)
        turned = jnp.concatenate([m_ref[b // 8, 0, rows, :], m_ref[b // 8, 1, rows, :]], axis=0).T
        for part, at in ((left_ref[b // 8, b % 8], 0), (turned, HALF), (right_ref[b // 8, b % 8], HALF + LANES)):
            part_high, part_low = split(part)
            high[b, pl.ds(at, part.shape[0]), :] = part_high
            low[b, pl.ds(at, part.shape[0]), :] = part_low
    left = iota((FB, LANES), 1) < 64
    for b in range(16):
        rows = pl.ds(b % 8 * FB, FB)
        for ref, at in ((r_ref, 0), (m_ref, LANES)):
            reals, imags = split(ref[b // 8, 0, rows, :]), split(ref[b // 8, 1, rows, :])
            for real, imag, out in ((reals[0], imags[0], w_high), (reals[1], imags[1], w_low)):
                real_turn, imag_turn = pltpu.roll(real, 64, 1), pltpu.roll(imag, 64, 1)
                pieces = (
                    jnp.where(left, real, imag_turn),
                    jnp.where(left, imag, -real_turn),
                    jnp.where(left, real_turn, imag),
                    jnp.where(left, imag_turn, -real),
                )
                for k, piece in enumerate(pieces):
                    out[b, pl.ds(k * FB, FB), pl.ds(at, LANES)] = piece
    row = iota((LANES, LANES), 0)
    inner = iota((LANES, LANES), 1) % 64
    band = row - inner
    grad_mask = (band >= 1) & (band <= 64)
    auto_mask = (band >= -31) & (band <= 32)
    tail_mask = ((band <= 95) & (inner < HALF))[96:]
    for b in range(16):
        lead = jnp.concatenate([high[b, 0:128, :], high[b, 64:192, :]], axis=1)
        rest = jnp.concatenate([low[b, 0:128, :], low[b, 64:192, :]], axis=1)
        table = mm(lead, w_high[b]) + mm(lead, w_low[b]) + mm(rest, w_high[b])
        grad, auto = table[:, :LANES], table[:, LANES:]
        for kind, part, mask, start, offset in (
            (0, grad, grad_mask, 0, 0),
            (1, auto, auto_mask, 0, HALF),
            (2, auto[96:], tail_mask, 96, HALF),
        ):
            part = jnp.where(mask, part, 0.0)
            total = None
            for g in range(part.shape[0] // 8):
                piece = pltpu.roll(part[g * 8 : g * 8 + 8], (offset - start - g * 8) % LANES, 1)
                total = piece if total is None else total + piece
            acc[kind, pl.ds(step * 16 + b, 1)] = total[None]

    @pl.when(step == shots // 2 - 1)
    def _():
        count = shots * 8
        sums = []
        for kind in range(3):
            total = acc[kind].reshape(count * 8, LANES)
            level = iota(total.shape, 0)
            for bit in (1, 2, 4):
                total = jnp.where(level // bit % 2 == 1, pltpu.roll(total, LANES - bit, 1), total)
            sums.append(jnp.sum(total.reshape(count, 8, LANES), axis=1))
        flip = ((iota((LANES, LANES), 0) + iota((LANES, LANES), 1)) % LANES == 0).astype(f32)
        flip = jnp.where(iota((LANES, LANES), 0) < 64, -flip, flip)
        auto = sums[1] + exact(sums[2], flip, ((1,), (0,)))
        for y in range(4):
            for x in range(4):
                for c in range(2):
                    place, k = number(y, x, c), (c * 4 + y) * 8
                    out_ref[place, 0:8, :] = sums[0][k : k + 8]
                    out_ref[place, 8:16, :] = auto[k : k + 8]


def corr(shots, multiples, recorded, left, right):
    return pl.pallas_call(
        lambda *refs: corr_kernel(shots, *refs),
        grid=(shots // 2,),
        in_specs=[field_spec(), field_spec(), edge_spec(), edge_spec()],
        out_specs=pl.BlockSpec((32, 16, LANES), lambda s: (0, 0, 0)),
        out_shape=jax.ShapeDtypeStruct((32, 16, LANES), f32),
        scratch_shapes=[
            pltpu.VMEM((16, 192, LANES), bf16),
            pltpu.VMEM((16, 192, LANES), bf16),
            pltpu.VMEM((16, 256, 256), bf16),
            pltpu.VMEM((16, 256, 256), bf16),
            pltpu.VMEM((3, shots * 8, 8, LANES), f32),
        ],
        compiler_params=pltpu.CompilerParams(vmem_limit_bytes=60 * 2**20),
        name="corr",
    )(multiples, recorded, left, right)


def solve_kernel(weight, z_ref, *refs):
    sums_refs, (out_ref, lags, table, vec) = refs[:4], refs[4:]
    grad_rows = jnp.concatenate([ref[0:8, :] for ref in sums_refs], axis=0)
    auto_rows = jnp.concatenate([ref[8:16, :] for ref in sums_refs], axis=0)
    turn = lambda value: pltpu.roll(value, 64, 1)
    lane = iota((TAPS, LANES), 1)
    row = iota((TAPS, LANES), 0)
    group = lane // HALF
    place = lane % HALF
    block = (place + z_ref[0] * 8) % HALF
    stacked = jnp.concatenate(
        [grad_rows, turn(grad_rows), turn(grad_rows), grad_rows], axis=0
    )
    pick = (lane == LANES - 1 - row).astype(f32)
    grad = exact(pick, stacked, ((1,), (1,)))
    lag = iota((LANES, LANES), 0) - 64
    pick = (iota((LANES, LANES), 1) == jnp.abs(lag)).astype(f32)
    stacked = jnp.concatenate(
        [auto_rows, turn(auto_rows), auto_rows, turn(auto_rows)], axis=0
    )
    made = exact(pick, stacked, ((1,), (1,)))
    odd = iota((LANES, LANES), 1) // HALF % 2 == 1
    lags[0:LANES, :] = jnp.where(odd & (lag < 0), -made, made)
    for a in range(HALF):
        part = jnp.concatenate(
            [ref[pl.ds(16 + a * 8, 8), :] for ref in sums_refs], axis=0
        )
        other = turn(part)
        turned = jnp.concatenate([part, other, part, other], axis=0).T
        table[a] = turned[:TAPS]

    flip = jnp.where(group == 3, -1.0, 1.0)
    even = group % 2 == 0

    def apply(vector):
        vec[...] = vector
        total = jnp.zeros((TAPS, LANES), f32)
        for k in range(TAPS):
            total = total + lags[64 - k : 128 - k, :] * vec[k : k + 1, :]
        low = jnp.zeros((HALF, LANES), f32)
        high = jnp.zeros((HALF, LANES), f32)
        for a in range(HALF):
            low = low + table[a, :HALF] * vec[a : a + 1, :]
            high = high + table[a, HALF:] * vec[HALF + a : HALF + a + 1, :]
        total = (total - jnp.concatenate([low, high], axis=0)) * flip
        total = total + pltpu.roll(total, LANES - HALF, 1)
        return jnp.where(even, total, pltpu.roll(total, LANES - HALF, 1))

    def bend(vector):
        before = jnp.where(place == 0, pltpu.roll(vector, 97, 1), pltpu.roll(vector, 1, 1))
        after = jnp.where(
            place == HALF - 1, pltpu.roll(vector, 31, 1), pltpu.roll(vector, 127, 1)
        )
        before = jnp.where(block == 0, 0.0, before)
        after = jnp.where(block == HALF - 1, 0.0, after)
        return 2.0 * vector - before - after

    def inner(left, right):
        return 0.5 * jnp.sum(left * right, keepdims=True)

    direction = grad
    taps = jnp.zeros_like(grad)
    norm = inner(grad, grad)
    for step in range(ITERS):
        if step > 0:
            norm_next = inner(grad, grad)
            direction = grad + (norm_next / norm) * direction
            norm = norm_next
        bent = apply(direction) + weight * bend(direction)
        length = norm / inner(direction, bent)
        taps = taps + length * direction
        grad = grad - length * bent
    pick = ((iota((TAPS, LANES), 1) % 64) == TAPS - 1 - row).astype(f32)
    made = exact(taps, pick, ((0,), (0,)))
    made = jnp.where(iota((8, LANES), 1) < 64, made[:8], made[HALF : HALF + 8])
    for k in range(8):
        out_ref[k] = made


def solve(weight, z, parts):
    return pl.pallas_call(
        lambda *refs: solve_kernel(weight, *refs),
        in_specs=[pl.BlockSpec(memory_space=pltpu.SMEM)]
        + [pl.BlockSpec(memory_space=pltpu.VMEM)] * 4,
        out_shape=jax.ShapeDtypeStruct((8, 8, LANES), f32),
        scratch_shapes=[
            pltpu.VMEM((LANES, LANES), f32),
            pltpu.VMEM((HALF, TAPS, LANES), f32),
            pltpu.VMEM((TAPS, LANES), f32),
        ],
        compiler_params=pltpu.CompilerParams(vmem_limit_bytes=8 * 2**20),
        name="solve",
    )(z, *parts)


def subtract_kernel(
    m_ref, r_ref, left_ref, right_ref, taps_ref, out_ref, taps_out_ref, lead, weights
):
    lane = iota((LANES, LANES), 1)
    for b in range(0, 16, 2):
        halo = jnp.concatenate(
            [
                right_ref[b // 8, b % 8 + 1],
                left_ref[b // 8, b % 8 + 1],
                right_ref[b // 8, b % 8],
                left_ref[b // 8, b % 8],
            ], axis=0
        ).T
        halos = split(halo)
        for odd in range(2):
            rows = pl.ds((b % 8 + odd) * FB, FB)
            field = jnp.concatenate([m_ref[b // 8, 0, rows, :], m_ref[b // 8, 1, rows, :]], axis=0)
            for k, (part, ends) in enumerate(zip(split(field), halos)):
                turned = pltpu.roll(part, 64, 1)
                if odd:
                    windows = (
                        jnp.where((lane >= 32) & (lane < 64), ends, turned),
                        jnp.where(lane < 32, ends, part),
                    )
                else:
                    windows = (
                        jnp.where(lane >= 96, ends, part),
                        jnp.where((lane >= 64) & (lane < 96), ends, turned),
                    )
                for j, window in enumerate(windows):
                    at = pl.ds(k * LANES + j * FB, FB)
                    lead[b + odd, at, pl.ds(0, LANES)] = window[:FB]
                    lead[b + odd, at, pl.ds(LANES, LANES)] = window[FB:]
    first = iota((1, LANES), 1) < 64
    masks = []
    for odd in range(2):
        spot = (iota((LANES, LANES), 0) + (96 if odd else 32)) % LANES
        band = spot - lane % 64
        masks.append((band >= 1) & (band <= 64))
    for b in range(16):
        mask, shift = masks[b % 2], (32 if b % 2 else 96)
        taps = taps_ref[b // 8, pl.ds(b % 8, 1), :]
        swapped = pltpu.roll(taps, 64, 1)
        swapped = jnp.where(first, -swapped, swapped)
        for j, line in enumerate((taps, swapped)):
            spread = jnp.broadcast_to(line, (LANES, LANES))
            spread = pltpu.roll(spread, shift, 1, stride=1, stride_axis=0)
            for k, part in enumerate(split(jnp.where(mask, spread, 0.0))):
                weights[b, pl.ds(j * LANES, LANES), pl.ds(k * LANES, LANES)] = part
    half = iota((FB, LANES), 1) < 64
    for b in range(16):
        rows = pl.ds(b % 8 * FB, FB)
        made = mm(lead[b], weights[b])
        made = (made[:LANES, :LANES] + made[LANES:, :LANES]) + (
            made[:LANES, LANES:] + made[LANES:, LANES:]
        )
        made0, made1 = made[:FB], made[FB:]
        real = jnp.where(half, made0, pltpu.roll(made1, 64, 1))
        imag = jnp.where(half, pltpu.roll(made0, 64, 1), made1)
        out_ref[b // 8, 0, rows, :] = r_ref[b // 8, 0, rows, :] - real
        out_ref[b // 8, 1, rows, :] = r_ref[b // 8, 1, rows, :] - imag
    for shot in range(2):
        taps_out_ref[shot, 0] = taps_ref[shot, :, :TAPS]
        taps_out_ref[shot, 1] = taps_ref[shot, :, TAPS:]


def subtract(multiples, recorded, left, right, taps):
    shots = multiples.shape[0]
    return pl.pallas_call(
        subtract_kernel,
        grid=(shots // 2,),
        in_specs=[
            field_spec(),
            field_spec(),
            edge_spec(),
            edge_spec(),
            pl.BlockSpec((2, 8, LANES), lambda s: (s, 0, 0)),
        ],
        out_specs=[field_spec(), pl.BlockSpec((2, 2, 8, TAPS), lambda s: (s, 0, 0, 0))],
        out_shape=[
            jax.ShapeDtypeStruct(recorded.shape, f32),
            jax.ShapeDtypeStruct((shots, 2, 8, TAPS), f32),
        ],
        scratch_shapes=[
            pltpu.VMEM((16, 256, 256), bf16),
            pltpu.VMEM((16, 256, 256), bf16),
        ],
        compiler_params=pltpu.CompilerParams(vmem_limit_bytes=60 * 2**20),
        name="subtract",
    )(multiples, recorded, left, right, taps)


def number(y, x, c):
    return (y * 4 + x) * 2 + c


def spread(value, axis, step, only=None):
    pairs = []
    for y in range(4):
        for x in range(4):
            for c in range(2):
                at = {"y": y, "x": x}
                to = dict(at)
                to[axis] = (at[axis] + step) % 4
                if only is None or only(y, x):
                    pairs.append((number(y, x, c), number(to["y"], to["x"], c)))
    return lax.ppermute(value, TRACE, pairs)


def across(value, moves):
    pairs = [
        (number(y, a, c), number(y, b, c)) for y in range(4) for a, b in moves for c in range(2)
    ]
    return lax.ppermute(value, TRACE, pairs)


def body(recorded, multiples):
    shots = multiples.shape[0]
    half = shots // 2
    y, x, c = (lax.axis_index(name) for name in TRACE)
    z = lax.axis_index("z")
    place = number(y, x, c)
    on = jnp.where(place == 0, 1, jnp.where(place == 31, 2, 0)).astype(jnp.int32)[None]
    up = [(i, i + 1) for i in range(31)]
    down = [(i + 1, i) for i in range(31)]
    first, last = pack(0, shots, multiples)
    left = lax.ppermute(last, TRACE, up)
    right = lax.ppermute(first, TRACE, down)
    ends = edges(on, first, last)

    ends = ends.reshape(2, half, 8, HALF, LANES)
    other = jnp.where(c == 0, ends[1], ends[0])
    mine = jnp.where(c == 0, ends[0], ends[1])
    mine = mine + lax.ppermute(other, TRACE, [(0, 1), (31, 30)])
    edge = lax.dynamic_index_in_dim(mine, y, 0, keepdims=False)
    for step in range(1, 4):
        sent = lax.dynamic_index_in_dim(mine, (y + step) % 4, 0, keepdims=False)
        edge = edge + spread(sent, "y", step, lambda y, x: (y, x) in ((0, 0), (3, 3)))
    edge = edge + across(edge, ((0, 2), (3, 1)))
    edge = edge + across(edge, ((0, 1), (2, 3), (3, 2), (1, 0)))
    edge = edge.transpose(1, 0, 2).reshape(8 * HALF, LANES)
    along = [[(i, (i - step) % 4) for i in range(4)] for step in range(1, 4)]

    sums = corr(shots, multiples, recorded, left, right)
    sums = lax.all_to_all(sums, TRACE, 0, 0, tiled=True).sum(axis=0)
    own = jnp.concatenate([sums, edge], axis=0)
    parts = [own] + [lax.ppermute(own, "z", pairs) for pairs in along]
    weight = 0.5 * FB * 4096
    taps = solve(weight, z[None], parts)
    taps = lax.all_to_all(taps, ("c", "y"), 0, 0, tiled=True)
    return tuple(subtract(multiples, recorded, left, right, taps))


def solution(mesh):
    finer = Mesh(mesh.devices.reshape(4, 4, 4, 2), AXES)
    placed = P(None, None, "z", TRACE)
    return jax.shard_map(
        body,
        mesh=finer,
        in_specs=(placed, placed),
        out_specs=(placed, P(None, None, "z", None)),
        check_vma=False,
    )
```

```python
import jax
import jax.numpy as jnp
from jax import lax
from jax.experimental import pallas as pl
from jax.experimental.pallas import tpu as pltpu
from jax.sharding import Mesh
from jax.sharding import PartitionSpec as P


FB = 64
TAPS = 64
ITERS = 3
HALF = 32
LANES = 128
AXES = ("z", "y", "x", "c")
TRACE = ("y", "x", "c")

f32 = jnp.float32
bf16 = jnp.bfloat16


def split(value):
    high = value.astype(bf16)
    return high, (value - high.astype(f32)).astype(bf16)


def mm(left, right):
    return lax.dot_general(left, right, (((1,), (0,)), ((), ())), preferred_element_type=f32)


def iota(shape, axis):
    return lax.broadcasted_iota(jnp.int32, shape, axis)


def mm_t(left, right):
    return lax.dot_general(left, right, (((1,), (1,)), ((), ())), preferred_element_type=f32)


def exact(left, right, dims):
    return lax.dot_general(
        left, right, (dims, ((), ())), precision=lax.Precision.HIGHEST,
        preferred_element_type=f32,
    )


def field_spec():
    return pl.BlockSpec((2, 2, 512, LANES), lambda s: (s, 0, 0, 0))


def edge_spec():
    return pl.BlockSpec((2, 8, HALF, LANES), lambda s: (s, 0, 0, 0))


def pack_kernel(m_ref, left_ref, right_ref):
    for shot in range(4):
        for b in range(8):
            rows = pl.ds(b * FB, FB)
            turned = jnp.concatenate(
                [m_ref[shot, 0, rows, :], m_ref[shot, 1, rows, :]], axis=0
            ).T
            left_ref[shot, b] = turned[:HALF]
            right_ref[shot, b] = turned[LANES - HALF :]


def pack(first, shots, multiples):
    shape = jax.ShapeDtypeStruct((shots, 8, HALF, LANES), f32)
    edge = pl.BlockSpec((4, 8, HALF, LANES), lambda s: (s, 0, 0, 0))
    return pl.pallas_call(
        pack_kernel,
        grid=(shots // 4,),
        in_specs=[pl.BlockSpec((4, 2, 512, LANES), lambda s: (s + first // 4, 0, 0, 0))],
        out_specs=[edge, edge],
        out_shape=[shape, shape],
        name="pack",
    )(multiples)


def edges_side(shots, turn, is_left, edge_ref, out_ref):
    lane = iota((HALF, LANES), 1)
    home = (lane % 64 >= HALF) if is_left else (lane % 64 < HALF)
    spot = lane % HALF
    sign = jnp.where(lane < 64, 1.0, -1.0)

    def load(shot, b):
        if is_left:
            return edge_ref[shot, b]
        return jnp.concatenate(
            [edge_ref[shot, b, 1:, :], jnp.zeros((1, LANES), f32)], axis=0
        )

    def one(group, carry):
        spots = [(group * 4 + k, b) for k in range(4) for b in range(0, 8, 2)]
        tables = []
        for shot, b in spots:
            here, there = load(shot, b), load(shot, b + 1)
            here_turn = pltpu.roll(here, 64, 1) * sign
            there_turn = pltpu.roll(there, 64, 1) * sign
            if is_left:
                against = [there, here, there_turn, here_turn]
            else:
                against = [here, there, here_turn, there_turn]
            against = split(jnp.concatenate(against, axis=0))
            rows = split(jnp.concatenate([here, there], axis=0))
            made = (
                mm_t(rows[0], against[0]) + mm_t(rows[0], against[1]) + mm_t(rows[1], against[0])
            )
            tables.append(jnp.where(home, made[:HALF], made[HALF:]))
        for step in (1, 2, 4, 8, 16):
            fill = jnp.zeros((step, LANES), f32)
            inside = (spot >= step) if is_left else (spot < HALF - step)
            for k, table in enumerate(tables):
                if is_left:
                    moved = jnp.concatenate([fill, pltpu.roll(table, step, 1)[:-step]], axis=0)
                else:
                    moved = jnp.concatenate(
                        [pltpu.roll(table, LANES - step, 1)[step:], fill], axis=0
                    )
                tables[k] = table + jnp.where(inside, moved, 0.0)
        for (shot, b), table in zip(spots, tables):
            to = lax.rem(shot + turn, shots)
            out_ref[to, b] = jnp.where(home, table, 0.0)
            other = pltpu.roll(table, HALF if is_left else LANES - HALF, 1)
            out_ref[to, b + 1] = jnp.where(home, other, 0.0)
        return carry

    lax.fori_loop(0, shots // 4, one, 0)


def edges_kernel(shots, on_ref, left_ref, right_ref, out_ref):
    @pl.when(on_ref[0] == 0)
    def _():
        out_ref[...] = jnp.zeros_like(out_ref)

    @pl.when(on_ref[0] == 1)
    def _():
        edges_side(shots, on_ref[1], True, left_ref, out_ref)

    @pl.when(on_ref[0] == 2)
    def _():
        edges_side(shots, on_ref[1], False, right_ref, out_ref)


def edges(on, first, last):
    shots = first.shape[0]
    return pl.pallas_call(
        lambda *refs: edges_kernel(shots, *refs),
        in_specs=[pl.BlockSpec(memory_space=pltpu.SMEM)]
        + [pl.BlockSpec(memory_space=pltpu.VMEM)] * 2,
        out_shape=jax.ShapeDtypeStruct((shots, 8, HALF, LANES), f32),
        compiler_params=pltpu.CompilerParams(vmem_limit_bytes=8 * 2**20),
        name="edges",
    )(on, first, last)


def corr_kernel(shots, m_ref, r_ref, left_ref, right_ref, out_ref, high, low, w_high, w_low, acc):
    step = pl.program_id(0)
    for b in range(16):
        rows = pl.ds(b % 8 * FB, FB)
        turned = jnp.concatenate([m_ref[b // 8, 0, rows, :], m_ref[b // 8, 1, rows, :]], axis=0).T
        for part, at in ((left_ref[b // 8, b % 8], 0), (turned, HALF), (right_ref[b // 8, b % 8], HALF + LANES)):
            part_high, part_low = split(part)
            high[b, pl.ds(at, part.shape[0]), :] = part_high
            low[b, pl.ds(at, part.shape[0]), :] = part_low
    left = iota((FB, LANES), 1) < 64
    for b in range(16):
        rows = pl.ds(b % 8 * FB, FB)
        for ref, at in ((r_ref, 0), (m_ref, LANES)):
            reals, imags = split(ref[b // 8, 0, rows, :]), split(ref[b // 8, 1, rows, :])
            for real, imag, out in ((reals[0], imags[0], w_high), (reals[1], imags[1], w_low)):
                real_turn, imag_turn = pltpu.roll(real, 64, 1), pltpu.roll(imag, 64, 1)
                pieces = (
                    jnp.where(left, real, imag_turn),
                    jnp.where(left, imag, -real_turn),
                    jnp.where(left, real_turn, imag),
                    jnp.where(left, imag_turn, -real),
                )
                for k, piece in enumerate(pieces):
                    out[b, pl.ds(k * FB, FB), pl.ds(at, LANES)] = piece
    row = iota((LANES, LANES), 0)
    inner = iota((LANES, LANES), 1) % 64
    band = row - inner
    grad_mask = (band >= 1) & (band <= 64)
    auto_mask = (band >= -31) & (band <= 32)
    tail_mask = ((band <= 95) & (inner < HALF))[96:]
    for b in range(16):
        lead = jnp.concatenate([high[b, 0:128, :], high[b, 64:192, :]], axis=1)
        rest = jnp.concatenate([low[b, 0:128, :], low[b, 64:192, :]], axis=1)
        table = mm(lead, w_high[b]) + mm(lead, w_low[b]) + mm(rest, w_high[b])
        grad, auto = table[:, :LANES], table[:, LANES:]
        for kind, part, mask, start, offset in (
            (0, grad, grad_mask, 0, 0),
            (1, auto, auto_mask, 0, HALF),
            (2, auto[96:], tail_mask, 96, HALF),
        ):
            part = jnp.where(mask, part, 0.0)
            total = None
            for g in range(part.shape[0] // 8):
                piece = pltpu.roll(part[g * 8 : g * 8 + 8], (offset - start - g * 8) % LANES, 1)
                total = piece if total is None else total + piece
            acc[kind, pl.ds(step * 16 + b, 1)] = total[None]

    @pl.when(step == shots // 2 - 1)
    def _():
        count = shots * 8
        sums = []
        for kind in range(3):
            total = acc[kind].reshape(count * 8, LANES)
            level = iota(total.shape, 0)
            for bit in (1, 2, 4):
                total = jnp.where(level // bit % 2 == 1, pltpu.roll(total, LANES - bit, 1), total)
            sums.append(jnp.sum(total.reshape(count, 8, LANES), axis=1))
        flip = ((iota((LANES, LANES), 0) + iota((LANES, LANES), 1)) % LANES == 0).astype(f32)
        flip = jnp.where(iota((LANES, LANES), 0) < 64, -flip, flip)
        auto = sums[1] + exact(sums[2], flip, ((1,), (0,)))
        for y in range(4):
            for x in range(4):
                for c in range(2):
                    place, k = number(y, x, c), (c * 4 + y) * 8
                    out_ref[place, 0:8, :] = sums[0][k : k + 8]
                    out_ref[place, 8:16, :] = auto[k : k + 8]


def corr(shots, multiples, recorded, left, right):
    return pl.pallas_call(
        lambda *refs: corr_kernel(shots, *refs),
        grid=(shots // 2,),
        in_specs=[field_spec(), field_spec(), edge_spec(), edge_spec()],
        out_specs=pl.BlockSpec((32, 16, LANES), lambda s: (0, 0, 0)),
        out_shape=jax.ShapeDtypeStruct((32, 16, LANES), f32),
        scratch_shapes=[
            pltpu.VMEM((16, 192, LANES), bf16),
            pltpu.VMEM((16, 192, LANES), bf16),
            pltpu.VMEM((16, 256, 256), bf16),
            pltpu.VMEM((16, 256, 256), bf16),
            pltpu.VMEM((3, shots * 8, 8, LANES), f32),
        ],
        compiler_params=pltpu.CompilerParams(vmem_limit_bytes=60 * 2**20),
        name="corr",
    )(multiples, recorded, left, right)


def solve_kernel(weight, z_ref, *refs):
    sums_refs, (out_ref, lags, table, vec) = refs[:4], refs[4:]
    grad_rows = jnp.concatenate([ref[0:8, :] for ref in sums_refs], axis=0)
    auto_rows = jnp.concatenate([ref[8:16, :] for ref in sums_refs], axis=0)
    turn = lambda value: pltpu.roll(value, 64, 1)
    lane = iota((TAPS, LANES), 1)
    row = iota((TAPS, LANES), 0)
    group = lane // HALF
    place = lane % HALF
    block = (place + z_ref[0] * 8) % HALF
    stacked = jnp.concatenate(
        [grad_rows, turn(grad_rows), turn(grad_rows), grad_rows], axis=0
    )
    pick = (lane == LANES - 1 - row).astype(f32)
    grad = exact(pick, stacked, ((1,), (1,)))
    lag = iota((LANES, LANES), 0) - 64
    pick = (iota((LANES, LANES), 1) == jnp.abs(lag)).astype(f32)
    stacked = jnp.concatenate(
        [auto_rows, turn(auto_rows), auto_rows, turn(auto_rows)], axis=0
    )
    made = exact(pick, stacked, ((1,), (1,)))
    odd = iota((LANES, LANES), 1) // HALF % 2 == 1
    lags[0:LANES, :] = jnp.where(odd & (lag < 0), -made, made)
    for a in range(HALF):
        part = jnp.concatenate(
            [ref[pl.ds(16 + a * 8, 8), :] for ref in sums_refs], axis=0
        )
        other = turn(part)
        turned = jnp.concatenate([part, other, part, other], axis=0).T
        table[a] = turned[:TAPS]

    flip = jnp.where(group == 3, -1.0, 1.0)
    even = group % 2 == 0

    def apply(vector):
        vec[...] = vector
        total = jnp.zeros((TAPS, LANES), f32)
        for k in range(TAPS):
            total = total + lags[64 - k : 128 - k, :] * vec[k : k + 1, :]
        low = jnp.zeros((HALF, LANES), f32)
        high = jnp.zeros((HALF, LANES), f32)
        for a in range(HALF):
            low = low + table[a, :HALF] * vec[a : a + 1, :]
            high = high + table[a, HALF:] * vec[HALF + a : HALF + a + 1, :]
        total = (total - jnp.concatenate([low, high], axis=0)) * flip
        total = total + pltpu.roll(total, LANES - HALF, 1)
        return jnp.where(even, total, pltpu.roll(total, LANES - HALF, 1))

    def bend(vector):
        before = jnp.where(place == 0, pltpu.roll(vector, 97, 1), pltpu.roll(vector, 1, 1))
        after = jnp.where(
            place == HALF - 1, pltpu.roll(vector, 31, 1), pltpu.roll(vector, 127, 1)
        )
        before = jnp.where(block == 0, 0.0, before)
        after = jnp.where(block == HALF - 1, 0.0, after)
        return 2.0 * vector - before - after

    def inner(left, right):
        return 0.5 * jnp.sum(left * right, keepdims=True)

    direction = grad
    taps = jnp.zeros_like(grad)
    norm = inner(grad, grad)
    for step in range(ITERS):
        if step > 0:
            norm_next = inner(grad, grad)
            direction = grad + (norm_next / norm) * direction
            norm = norm_next
        bent = apply(direction) + weight * bend(direction)
        length = norm / inner(direction, bent)
        taps = taps + length * direction
        grad = grad - length * bent
    pick = ((iota((TAPS, LANES), 1) % 64) == TAPS - 1 - row).astype(f32)
    made = exact(taps, pick, ((0,), (0,)))
    made = jnp.where(iota((8, LANES), 1) < 64, made[:8], made[HALF : HALF + 8])
    for k in range(8):
        out_ref[k] = made


def solve(weight, z, parts):
    return pl.pallas_call(
        lambda *refs: solve_kernel(weight, *refs),
        in_specs=[pl.BlockSpec(memory_space=pltpu.SMEM)]
        + [pl.BlockSpec(memory_space=pltpu.VMEM)] * 4,
        out_shape=jax.ShapeDtypeStruct((8, 8, LANES), f32),
        scratch_shapes=[
            pltpu.VMEM((LANES, LANES), f32),
            pltpu.VMEM((HALF, TAPS, LANES), f32),
            pltpu.VMEM((TAPS, LANES), f32),
        ],
        compiler_params=pltpu.CompilerParams(vmem_limit_bytes=8 * 2**20),
        name="solve",
    )(z, *parts)


def subtract_kernel(
    m_ref, r_ref, left_ref, right_ref, taps_ref, out_ref, taps_out_ref, lead, weights
):
    lane = iota((LANES, LANES), 1)
    for b in range(0, 16, 2):
        halo = jnp.concatenate(
            [
                right_ref[b // 8, b % 8 + 1],
                left_ref[b // 8, b % 8 + 1],
                right_ref[b // 8, b % 8],
                left_ref[b // 8, b % 8],
            ], axis=0
        ).T
        halos = split(halo)
        for odd in range(2):
            rows = pl.ds((b % 8 + odd) * FB, FB)
            field = jnp.concatenate([m_ref[b // 8, 0, rows, :], m_ref[b // 8, 1, rows, :]], axis=0)
            for k, (part, ends) in enumerate(zip(split(field), halos)):
                turned = pltpu.roll(part, 64, 1)
                if odd:
                    windows = (
                        jnp.where((lane >= 32) & (lane < 64), ends, turned),
                        jnp.where(lane < 32, ends, part),
                    )
                else:
                    windows = (
                        jnp.where(lane >= 96, ends, part),
                        jnp.where((lane >= 64) & (lane < 96), ends, turned),
                    )
                for j, window in enumerate(windows):
                    at = pl.ds(k * LANES + j * FB, FB)
                    lead[b + odd, at, pl.ds(0, LANES)] = window[:FB]
                    lead[b + odd, at, pl.ds(LANES, LANES)] = window[FB:]
    first = iota((1, LANES), 1) < 64
    masks = []
    for odd in range(2):
        spot = (iota((LANES, LANES), 0) + (96 if odd else 32)) % LANES
        band = spot - lane % 64
        masks.append((band >= 1) & (band <= 64))
    for b in range(16):
        mask, shift = masks[b % 2], (32 if b % 2 else 96)
        taps = taps_ref[b // 8, pl.ds(b % 8, 1), :]
        swapped = pltpu.roll(taps, 64, 1)
        swapped = jnp.where(first, -swapped, swapped)
        for j, line in enumerate((taps, swapped)):
            spread = jnp.broadcast_to(line, (LANES, LANES))
            spread = pltpu.roll(spread, shift, 1, stride=1, stride_axis=0)
            for k, part in enumerate(split(jnp.where(mask, spread, 0.0))):
                weights[b, pl.ds(j * LANES, LANES), pl.ds(k * LANES, LANES)] = part
    half = iota((FB, LANES), 1) < 64
    for b in range(16):
        rows = pl.ds(b % 8 * FB, FB)
        made = mm(lead[b], weights[b])
        made = (made[:LANES, :LANES] + made[LANES:, :LANES]) + (
            made[:LANES, LANES:] + made[LANES:, LANES:]
        )
        made0, made1 = made[:FB], made[FB:]
        real = jnp.where(half, made0, pltpu.roll(made1, 64, 1))
        imag = jnp.where(half, pltpu.roll(made0, 64, 1), made1)
        out_ref[b // 8, 0, rows, :] = r_ref[b // 8, 0, rows, :] - real
        out_ref[b // 8, 1, rows, :] = r_ref[b // 8, 1, rows, :] - imag
    for shot in range(2):
        taps_out_ref[shot, 0] = taps_ref[shot, :, :TAPS]
        taps_out_ref[shot, 1] = taps_ref[shot, :, TAPS:]


def subtract(multiples, recorded, left, right, taps):
    shots = multiples.shape[0]
    return pl.pallas_call(
        subtract_kernel,
        grid=(shots // 2,),
        in_specs=[
            field_spec(),
            field_spec(),
            edge_spec(),
            edge_spec(),
            pl.BlockSpec((2, 8, LANES), lambda s: (s, 0, 0)),
        ],
        out_specs=[field_spec(), pl.BlockSpec((2, 2, 8, TAPS), lambda s: (s, 0, 0, 0))],
        out_shape=[
            jax.ShapeDtypeStruct(recorded.shape, f32),
            jax.ShapeDtypeStruct((shots, 2, 8, TAPS), f32),
        ],
        scratch_shapes=[
            pltpu.VMEM((16, 256, 256), bf16),
            pltpu.VMEM((16, 256, 256), bf16),
        ],
        compiler_params=pltpu.CompilerParams(vmem_limit_bytes=60 * 2**20),
        name="subtract",
    )(multiples, recorded, left, right, taps)


def number(y, x, c):
    return (y * 4 + x) * 2 + c


def spread(value, axis, step, only=None):
    pairs = []
    for y in range(4):
        for x in range(4):
            for c in range(2):
                at = {"y": y, "x": x}
                to = dict(at)
                to[axis] = (at[axis] + step) % 4
                if only is None or only(y, x):
                    pairs.append((number(y, x, c), number(to["y"], to["x"], c)))
    return lax.ppermute(value, TRACE, pairs)


def across(value, moves):
    pairs = [
        (number(y, a, c), number(y, b, c)) for y in range(4) for a, b in moves for c in range(2)
    ]
    return lax.ppermute(value, TRACE, pairs)


def body(recorded, multiples):
    shots = multiples.shape[0]
    half = shots // 2
    y, x, c = (lax.axis_index(name) for name in TRACE)
    z = lax.axis_index("z")
    place = number(y, x, c)
    on = jnp.where(place == 0, 1, jnp.where(place == 31, 2, 0))
    on = jnp.stack([on, c * half]).astype(jnp.int32)
    up = [(i, i + 1) for i in range(31)]
    down = [(i + 1, i) for i in range(31)]
    first, last = pack(0, shots, multiples)
    left = lax.ppermute(last, TRACE, up)
    right = lax.ppermute(first, TRACE, down)
    ends = edges(on, first, last)

    mine, other = ends[:half], ends[half:]
    mine = mine + lax.ppermute(other, TRACE, [(0, 1), (31, 30)])
    edge = lax.dynamic_index_in_dim(mine, y, 0, keepdims=False)
    for step in range(1, 4):
        sent = lax.dynamic_index_in_dim(mine, (y + step) % 4, 0, keepdims=False)
        edge = edge + spread(sent, "y", step, lambda y, x: (y, x) in ((0, 0), (3, 3)))
    edge = edge + across(edge, ((0, 2), (3, 1)))
    edge = edge + across(edge, ((0, 1), (2, 3), (3, 2), (1, 0)))
    edge = edge.transpose(1, 0, 2).reshape(8 * HALF, LANES)
    along = [[(i, (i - step) % 4) for i in range(4)] for step in range(1, 4)]

    sums = corr(shots, multiples, recorded, left, right)
    sums = lax.all_to_all(sums, TRACE, 0, 0, tiled=True).sum(axis=0)
    own = jnp.concatenate([sums, edge], axis=0)
    parts = [own] + [lax.ppermute(own, "z", pairs) for pairs in along]
    weight = 0.5 * FB * 4096
    taps = solve(weight, z[None], parts)
    taps = lax.all_to_all(taps, ("c", "y"), 0, 0, tiled=True)
    return tuple(subtract(multiples, recorded, left, right, taps))


def solution(mesh):
    finer = Mesh(mesh.devices.reshape(4, 4, 4, 2), AXES)
    placed = P(None, None, "z", TRACE)
    return jax.shard_map(
        body,
        mesh=finer,
        in_specs=(placed, placed),
        out_specs=(placed, P(None, None, "z", None)),
        check_vma=False,
    )
```
